32 devices in a mesh: gz: 4 (over z), gy: 4 (over y, x), gx: 2 (over core).
Axes of the slice: x: 2, y: 2, z: 4, core: 2. Of those that a mesh axis runs over, the one named last changes fastest.
Arguments:
- rhs: float32 [16, 64, 8192], P('gz', 'gy', 'gx'), may hold values from -20 to 20
- guess: float32 [16, 64, 8192], P('gz', 'gy', 'gx'), may hold values from -0.6 to 0.6
- shifts: float32 [64], replicated, may hold values from 0.5 to 4
Outputs:
- normalized: float32 [16, 64, 8192], P('gz', 'gy', 'gx')
- gram_mean: float32 [64, 64], replicated
The draws below stay inside these ranges and needn't reach their ends.
All inputs are finite; a program needn't handle non-finite values.
Results may differ from the reference program's by a relative error of at most 0.000088.
Values sent between devices are 32-bit elements; how exact they have to be, the bound alone decides.
No kernel may reach another device: no remote copies, remote signals or barrier semaphores. Data moves between devices by JAX's collectives and lax.ppermute only.
A program may use at most 64 MiB of HBM per device.

```python
import math
import jax
import jax.numpy as jnp
from jax import lax

RHS = 64
NZ = 16
NY = 64
NX = 128
NCELLS = 131072


def draw_rhs(key, part):
    noise_key = jax.random.fold_in(key, 11)
    mix_key = jax.random.fold_in(key, 12)
    scale_key = jax.random.fold_in(key, 13)
    noise = jax.random.truncated_normal(noise_key, -4.0, 4.0, (NZ, NY, NX, RHS), jnp.float32)
    mixing = jnp.eye(RHS, dtype=jnp.float32) + 0.3 * jax.random.truncated_normal(mix_key, -3.0, 3.0, (RHS, RHS), jnp.float32)
    mixing = mixing / jnp.sqrt(1.0 + 0.09 * RHS)
    column_scale = jnp.exp(jax.random.uniform(scale_key, (RHS,), jnp.float32, jnp.log(0.3), jnp.log(3.0)))
    depth = jnp.arange(NZ, dtype=jnp.float32) / jnp.float32(max(NZ - 1, 1))
    z_scale = 10.0 ** (depth - 1.0)
    mixed = jnp.einsum('zyxk,kj->zyxj', noise, mixing)
    values = jnp.clip(mixed * column_scale * z_scale[:, None, None, None], -20.0, 20.0)
    return values.reshape(NZ, NY, NX * RHS)


def block_levels(stream_key, extent, pieces, low, top_value):
    def one(axis_at, shards_of):
        draws = jax.random.uniform(jax.random.fold_in(jax.random.fold_in(stream_key, 6), axis_at), (shards_of,), jnp.float32, low / len(pieces), top_value / len(pieces))
        return jnp.repeat(jnp.exp(draws), extent[axis_at] // shards_of).reshape((-1,) + (1,) * (len(extent) - axis_at - 1))

    gain = one(*pieces[0])
    for cut in pieces[1:]:
        gain = gain * one(*cut)
    return gain


def bell_draw(key, shape, scale, limit, pieces=(), held_as=jnp.bfloat16):
    result = scale * jax.random.normal(key, shape, jnp.float32)
    if pieces:
        result = result * block_levels(key, shape, pieces, -0.22, 0.18)
    return jnp.clip(result, -limit, limit).astype(held_as)


def setup_inputs(seed: int = 0) -> dict:
    arg_keys = jax.random.split(jax.random.key(seed), 4)
    return {
        "rhs": draw_rhs(jax.random.fold_in(arg_keys[3], 71), 0),
        "guess": bell_draw(arg_keys[1], (NZ, NY, NX * RHS), 0.1, 0.6, ((0, 4), (1, 4), (2, 2)), jnp.float32),
        "shifts": jnp.clip(jnp.exp(jax.random.uniform(arg_keys[2], (RHS,), jnp.float32, math.log(0.5), math.log(4.0))), 0.5, 4.0),
    }


def reference(rhs, guess, shifts):
    b_cells = rhs.reshape(NZ, NY, NX, RHS)
    x_cells = guess.reshape(NZ, NY, NX, RHS)
    neighbours = jnp.roll(x_cells, 1, 0) + jnp.roll(x_cells, -1, 0)
    neighbours = neighbours + jnp.roll(x_cells, 1, 1) + jnp.roll(x_cells, -1, 1)
    neighbours = neighbours + jnp.roll(x_cells, 1, 2) + jnp.roll(x_cells, -1, 2)
    resid = b_cells - ((6.0 + shifts) * x_cells - neighbours)
    flattened = resid.reshape(-1, RHS)
    gram = lax.dot_general(flattened, flattened, (((0,), (0,)), ((), ())), precision=lax.Precision.HIGHEST, preferred_element_type=jnp.float32)
    gram_mean = gram / jnp.float32(NCELLS)
    inv_norm = lax.rsqrt(jnp.diagonal(gram_mean) + 1e-06)
    normalized = (resid * inv_norm).reshape(NZ, NY, NX * RHS)
    return (normalized, gram_mean)
```

```python
import jax
import jax.numpy as jnp
from jax import lax
from jax.sharding import PartitionSpec as P

AXES = ("gz", "gy", "gx")


def ring(array, axis, step):
    peers = lax.axis_size(axis)
    return lax.ppermute(array, axis, [(i, (i + step) % peers) for i in range(peers)])


def halos(array, axis, dim, width):
    length = array.shape[dim]
    last = lax.slice_in_dim(array, length - width, length, axis=dim)
    initial = lax.slice_in_dim(array, 0, width, axis=dim)
    return ring(last, axis, 1), ring(initial, axis, -1)


def pair_halos(array, axis, dim, width):
    if lax.axis_size(axis) != 2:
        return halos(array, axis, dim, width)
    length = array.shape[dim]
    last = lax.slice_in_dim(array, length - width, length, axis=dim)
    initial = lax.slice_in_dim(array, 0, width, axis=dim)
    both = ring(jnp.concatenate([last, initial], axis=dim), axis, 1)
    return (
        lax.slice_in_dim(both, 0, width, axis=dim),
        lax.slice_in_dim(both, width, 2 * width, axis=dim),
    )


def masks_of(devices):
    masks = [1]
    while 2 ** len(masks) < devices:
        masks.append(2 ** len(masks) + 1)
    return masks


def sum_over_all(value):
    devices = lax.axis_size(AXES)
    for mask in masks_of(devices):
        value = value + lax.ppermute(value, AXES, [(i, i ^ mask) for i in range(devices)])
    return value


def local(rhs, guess, shifts):
    z_cells, y_cells, lane_count = guess.shape
    columns = shifts.shape[0]
    x_cells = lane_count // columns
    z_before, z_after = halos(guess, "gz", 0, 1)
    y_before, y_after = halos(guess, "gy", 1, 1)
    x_before, x_after = pair_halos(guess, "gx", 2, columns)
    z_padded = jnp.concatenate([z_before, guess, z_after], axis=0)
    y_padded = jnp.concatenate([y_before, guess, y_after], axis=1)
    x_padded = jnp.concatenate([x_before, guess, x_after], axis=2)
    neighbours = z_padded[2:] + z_padded[:-2] + y_padded[:, 2:] + y_padded[:, :-2]
    neighbours = neighbours + x_padded[:, :, 2 * columns :] + x_padded[:, :, : -2 * columns]
    centre = jnp.tile(6.0 + shifts, x_cells)
    resid = rhs - (centre * guess - neighbours)
    flattened = resid.reshape(-1, columns)
    partial_gram = lax.dot_general(
        flattened,
        flattened,
        (((0,), (0,)), ((), ())),
        precision=lax.Precision.HIGHEST,
        preferred_element_type=jnp.float32,
    )
    gram = sum_over_all(partial_gram)
    total_cells = z_cells * y_cells * x_cells * lax.axis_size(AXES)
    gram_mean = gram / jnp.float32(total_cells)
    diagonal = jnp.sum(gram_mean * jnp.eye(columns, dtype=jnp.float32), axis=0)
    inverse_norm = lax.rsqrt(diagonal + 1e-06)
    normalized = resid * jnp.tile(inverse_norm, x_cells)
    return (normalized, gram_mean)


def solution(mesh):
    placed = (P("gz", "gy", "gx"), P("gz", "gy", "gx"), P())
    return jax.shard_map(
        local, mesh=mesh, in_specs=placed, out_specs=(P("gz", "gy", "gx"), P()), check_vma=False
    )
```

```python
import functools

import jax
import jax.numpy as jnp
from jax import lax
from jax.experimental import pallas as pl
from jax.experimental.pallas import tpu as pltpu
from jax.sharding import PartitionSpec as P


AXES = ("gz", "gy", "gx")
LANES = 128
VMEM = pl.BlockSpec(memory_space=pltpu.VMEM)


def ring(array, axis, step):
    peers = lax.axis_size(axis)
    return lax.ppermute(array, axis, [(i, (i + step) % peers) for i in range(peers)])


def faces(array, dim, width):
    length = array.shape[dim]
    last = lax.slice_in_dim(array, length - width, length, axis=dim)
    initial = lax.slice_in_dim(array, 0, width, axis=dim)
    return last, initial


def masks_of(devices):
    masks = [1]
    while 2 ** len(masks) < devices:
        masks.append(2 ** len(masks) + 1)
    return masks


def sum_over_all(value):
    devices = lax.axis_size(AXES)
    for mask in masks_of(devices):
        value = value + lax.ppermute(value, AXES, [(i, i ^ mask) for i in range(devices)])
    return value


def half_roll(tile):
    return pltpu.roll(tile, LANES // 2, axis=1)


def split_gram(tiles):
    block = jnp.concatenate(tiles, axis=0)
    hi = block.astype(jnp.bfloat16)
    lo = (block - hi.astype(jnp.float32)).astype(jnp.bfloat16)
    return lax.dot_general(
        hi,
        jnp.concatenate([hi, lo], axis=1),
        (((0,), (0,)), ((), ())),
        preferred_element_type=jnp.float32,
    )


def early(g_ref, b_ref, c_ref, yb_ref, ya_ref, xh_ref, l_ref, gram_ref):
    planes, rows, width = g_ref.shape
    chunks = width // LANES
    row = lax.broadcasted_iota(jnp.int32, (rows, LANES), 0)
    low = lax.broadcasted_iota(jnp.int32, (rows, LANES), 1) < LANES // 2
    centre = jnp.broadcast_to(c_ref[...], (rows, LANES))
    gram_ref[...] = jnp.zeros_like(gram_ref)

    def plane(z):
        xh = xh_ref[z]
        before, here = xh, half_roll(g_ref[z, :, pl.ds(0, LANES)])
        tiles = []
        for t in range(chunks):
            at = pl.ds(t * LANES, LANES)
            after = half_roll(g_ref[z, :, pl.ds((t + 1) * LANES, LANES)]) if t + 1 < chunks else xh
            x = g_ref[z, :, at]
            near = here + jnp.where(low, before, after)
            up = jnp.where(row == 0, yb_ref[z, :, at], pltpu.roll(x, 1, axis=0))
            down = jnp.where(row == rows - 1, ya_ref[z, :, at], pltpu.roll(x, rows - 1, axis=0))
            near = near + (up + down)
            if z > 0:
                near = near + g_ref[z - 1, :, at]
            if z < planes - 1:
                near = near + g_ref[z + 1, :, at]
            left = b_ref[z, :, at] - (centre * x - near)
            l_ref[z, :, at] = left
            tiles.append(left)
            before, here = here, after
        if 0 < z < planes - 1:
            gram_ref[...] += split_gram(tiles)

    for z in range(planes):
        plane(z)


def pack_gram(split):
    half, quarter = LANES // 2, LANES // 4
    hh, hl = split[:, :LANES], split[:, LANES:]
    full = hh + hl + hl.T
    low = lax.broadcasted_iota(jnp.int32, (quarter, LANES), 1) < half
    first = jnp.where(low, full[:quarter], half_roll(full[quarter:half]))
    second = jnp.where(
        low, half_roll(full[half : half + quarter]), full[half + quarter :]
    )
    return first + second


def late(l_ref, zb_ref, za_ref, g_ref, r_ref, p_ref):
    planes, _, width = l_ref.shape
    tiles = []
    for i, z, h_ref in ((0, 0, zb_ref), (1, planes - 1, za_ref)):
        for t in range(width // LANES):
            at = pl.ds(t * LANES, LANES)
            value = l_ref[z, :, at] + h_ref[0, :, at]
            r_ref[i, :, at] = value
            tiles.append(value)
    p_ref[...] = pack_gram(g_ref[...] + split_gram(tiles))


def final(cells, p_ref, l_ref, r_ref, n_ref, m_ref, buf, sem):
    planes, rows, width = l_ref.shape
    half, quarter = LANES // 2, LANES // 4
    mean = p_ref[...] / jnp.float32(cells)
    row = lax.broadcasted_iota(jnp.int32, (quarter, LANES), 0)
    lane = lax.broadcasted_iota(jnp.int32, (quarter, LANES), 1)
    own = (lane == row) | (lane == row + half + quarter)
    diagonal = jnp.sum(jnp.where(own, mean, 0.0), axis=0, keepdims=True)
    diagonal = diagonal + half_roll(diagonal)
    scale = jnp.broadcast_to(lax.rsqrt(diagonal + 1e-06), (rows, LANES))
    copies = []
    for z in range(planes):
        source = r_ref.at[0] if z == 0 else r_ref.at[1] if z == planes - 1 else l_ref.at[z]
        for t in range(width // LANES):
            at = pl.ds(t * LANES, LANES)
            buf[z, :, at] = source[:, at] * scale
        copy = pltpu.make_async_copy(buf.at[z], n_ref.at[z], sem.at[z])
        copy.start()
        copies.append(copy)
    m_ref[pl.ds(0, quarter), :] = mean[:, :half]
    m_ref[pl.ds(quarter, quarter), :] = half_roll(mean)[:, :half]
    for copy in copies:
        copy.wait()


def call(body, outs, cost, **kwargs):
    return pl.pallas_call(
        body,
        out_shape=outs,
        cost_estimate=pl.CostEstimate(flops=cost, bytes_accessed=1 << 20, transcendentals=0),
        compiler_params=pltpu.CompilerParams(vmem_limit_bytes=16 << 20),
        **kwargs,
    )


def local(rhs, guess, shifts):
    z_cells, y_cells, lane_count = guess.shape
    columns = shifts.shape[0]
    x_cells = lane_count // columns
    f32 = jnp.float32
    last, initial = faces(guess, 0, 1)
    z_before = ring(last, "gz", 1)
    z_after = ring(initial, "gz", -1)
    last, initial = faces(guess, 1, 1)
    y_before = ring(last, "gy", 1)
    y_after = ring(initial, "gy", -1)
    last, initial = faces(guess, 2, columns)
    if lax.axis_size("gx") == 2:
        x_halos = ring(jnp.concatenate([last, initial], axis=2), "gx", 1)
    else:
        x_halos = jnp.concatenate(
            [ring(last, "gx", 1), ring(initial, "gx", -1)], axis=2
        )
    centre = jnp.tile(6.0 + shifts, LANES // columns)[None]
    left, inner = call(
        early,
        (
            jax.ShapeDtypeStruct(guess.shape, f32),
            jax.ShapeDtypeStruct((LANES, 2 * LANES), f32),
        ),
        1 << 24,
        in_specs=[VMEM] * 6,
        out_specs=[VMEM] * 2,
    )(guess, rhs, centre, y_before, y_after, x_halos)
    outer, packed = call(
        late,
        (
            jax.ShapeDtypeStruct((2, y_cells, lane_count), f32),
            jax.ShapeDtypeStruct((columns // 2, LANES), f32),
        ),
        1 << 24,
        in_specs=[VMEM] * 4,
        out_specs=[VMEM] * 2,
    )(left, z_before, z_after, inner)
    packed = sum_over_all(packed)
    total_cells = z_cells * y_cells * x_cells * lax.axis_size(AXES)
    return call(
        functools.partial(final, total_cells),
        (
            jax.ShapeDtypeStruct(guess.shape, f32),
            jax.ShapeDtypeStruct((columns, columns), f32),
        ),
        1 << 22,
        in_specs=[VMEM] * 3,
        out_specs=[pl.BlockSpec(memory_space=pl.ANY), VMEM],
        scratch_shapes=[
            pltpu.VMEM(guess.shape, f32),
            pltpu.SemaphoreType.DMA((z_cells,)),
        ],
    )(packed, left, outer)


def solution(mesh):
    placed = (P("gz", "gy", "gx"), P("gz", "gy", "gx"), P())
    return jax.shard_map(
        local, mesh=mesh, in_specs=placed, out_specs=(P("gz", "gy", "gx"), P()), check_vma=False
    )
```

```python
import functools

import jax
import jax.numpy as jnp
from jax import lax
from jax.experimental import pallas as pl
from jax.experimental.pallas import tpu as pltpu
from jax.sharding import PartitionSpec as P


AXES = ("gz", "gy", "gx")
LANES = 128
VMEM = pl.BlockSpec(memory_space=pltpu.VMEM)


def ring(array, axis, step):
    peers = lax.axis_size(axis)
    return lax.ppermute(array, axis, [(i, (i + step) % peers) for i in range(peers)])


def faces(array, dim, width):
    length = array.shape[dim]
    last = lax.slice_in_dim(array, length - width, length, axis=dim)
    initial = lax.slice_in_dim(array, 0, width, axis=dim)
    return last, initial


def stages_of(devices):
    bits = [1 << k for k in range(1, (devices - 1).bit_length())]
    stages = [(1,)]
    for low, high in zip(bits[0::2], bits[1::2]):
        stages.append((low | high, high | 1, low | 1))
    if len(bits) % 2:
        stages.append((bits[-1] | 1,))
    return stages


def sum_over_all(value):
    devices = lax.axis_size(AXES)
    for masks in stages_of(devices):
        got = []
        for mask in masks:
            got.append(lax.ppermute(value, AXES, [(i, i ^ mask) for i in range(devices)]))
        if len(got) == 1:
            value = value + got[0]
        else:
            far, second, first = got
            value = (value + first) + (second + far)
    return value


def half_roll(tile):
    return pltpu.roll(tile, LANES // 2, axis=1)


def split_gram(tiles):
    block = jnp.concatenate(tiles, axis=0)
    hi = block.astype(jnp.bfloat16)
    lo = (block - hi.astype(jnp.float32)).astype(jnp.bfloat16)
    return lax.dot_general(
        hi,
        jnp.concatenate([hi, lo], axis=1),
        (((0,), (0,)), ((), ())),
        preferred_element_type=jnp.float32,
    )


def early(g_ref, b_ref, c_ref, yb_ref, ya_ref, xh_ref, l_ref, gram_ref):
    planes, rows, width = g_ref.shape
    chunks = width // LANES
    row = lax.broadcasted_iota(jnp.int32, (rows, LANES), 0)
    low = lax.broadcasted_iota(jnp.int32, (rows, LANES), 1) < LANES // 2
    centre = jnp.broadcast_to(c_ref[...], (rows, LANES))
    gram_ref[...] = jnp.zeros_like(gram_ref)

    def plane(z):
        xh = xh_ref[z]
        before, here = xh, half_roll(g_ref[z, :, pl.ds(0, LANES)])
        tiles = []
        for t in range(chunks):
            at = pl.ds(t * LANES, LANES)
            after = half_roll(g_ref[z, :, pl.ds((t + 1) * LANES, LANES)]) if t + 1 < chunks else xh
            x = g_ref[z, :, at]
            near = here + jnp.where(low, before, after)
            up = jnp.where(row == 0, yb_ref[z, :, at], pltpu.roll(x, 1, axis=0))
            down = jnp.where(row == rows - 1, ya_ref[z, :, at], pltpu.roll(x, rows - 1, axis=0))
            near = near + (up + down)
            if z > 0:
                near = near + g_ref[z - 1, :, at]
            if z < planes - 1:
                near = near + g_ref[z + 1, :, at]
            left = b_ref[z, :, at] - (centre * x - near)
            l_ref[z, :, at] = left
            tiles.append(left)
            before, here = here, after
        if 0 < z < planes - 1:
            gram_ref[...] += split_gram(tiles)

    for z in range(planes):
        plane(z)


def pack_gram(split):
    half, quarter = LANES // 2, LANES // 4
    hh, hl = split[:, :LANES], split[:, LANES:]
    full = hh + hl + hl.T
    low = lax.broadcasted_iota(jnp.int32, (quarter, LANES), 1) < half
    first = jnp.where(low, full[:quarter], half_roll(full[quarter:half]))
    second = jnp.where(
        low, half_roll(full[half : half + quarter]), full[half + quarter :]
    )
    return first + second


def late(l_ref, zb_ref, za_ref, g_ref, r_ref, p_ref):
    planes, _, width = l_ref.shape
    tiles = []
    for i, z, h_ref in ((0, 0, zb_ref), (1, planes - 1, za_ref)):
        for t in range(width // LANES):
            at = pl.ds(t * LANES, LANES)
            value = l_ref[z, :, at] + h_ref[0, :, at]
            r_ref[i, :, at] = value
            tiles.append(value)
    p_ref[...] = pack_gram(g_ref[...] + split_gram(tiles))


def final(cells, p_ref, l_ref, r_ref, n_ref, m_ref, buf, gram, sem):
    planes, rows, width = l_ref.shape
    half, quarter = LANES // 2, LANES // 4
    mean = p_ref[...] / jnp.float32(cells)
    gram[pl.ds(0, quarter), :] = mean[:, :half]
    gram[pl.ds(quarter, quarter), :] = half_roll(mean)[:, :half]
    copies = [pltpu.make_async_copy(gram, m_ref, sem.at[planes])]
    copies[0].start()
    row = lax.broadcasted_iota(jnp.int32, (quarter, LANES), 0)
    lane = lax.broadcasted_iota(jnp.int32, (quarter, LANES), 1)
    own = (lane == row) | (lane == row + half + quarter)
    diagonal = jnp.sum(jnp.where(own, mean, 0.0), axis=0, keepdims=True)
    diagonal = diagonal + half_roll(diagonal)
    scale = jnp.broadcast_to(lax.rsqrt(diagonal + 1e-06), (rows, LANES))
    for z in range(planes):
        source = r_ref.at[0] if z == 0 else r_ref.at[1] if z == planes - 1 else l_ref.at[z]
        for t in range(width // LANES):
            at = pl.ds(t * LANES, LANES)
            buf[z, :, at] = source[:, at] * scale
        copy = pltpu.make_async_copy(buf.at[z], n_ref.at[z], sem.at[z])
        copy.start()
        copies.append(copy)
    for copy in copies:
        copy.wait()


def call(body, outs, cost, **kwargs):
    return pl.pallas_call(
        body,
        out_shape=outs,
        cost_estimate=pl.CostEstimate(flops=cost, bytes_accessed=1 << 20, transcendentals=0),
        compiler_params=pltpu.CompilerParams(vmem_limit_bytes=16 << 20),
        **kwargs,
    )


def local(rhs, guess, shifts):
    z_cells, y_cells, lane_count = guess.shape
    columns = shifts.shape[0]
    x_cells = lane_count // columns
    f32 = jnp.float32
    last, initial = faces(guess, 0, 1)
    z_before = ring(last, "gz", 1)
    z_after = ring(initial, "gz", -1)
    last, initial = faces(guess, 1, 1)
    y_before = ring(last, "gy", 1)
    y_after = ring(initial, "gy", -1)
    last, initial = faces(guess, 2, columns)
    if lax.axis_size("gx") == 2:
        x_halos = ring(jnp.concatenate([last, initial], axis=2), "gx", 1)
    else:
        x_halos = jnp.concatenate(
            [ring(last, "gx", 1), ring(initial, "gx", -1)], axis=2
        )
    centre = jnp.tile(6.0 + shifts, LANES // columns)[None]
    left, inner = call(
        early,
        (
            jax.ShapeDtypeStruct(guess.shape, f32),
            jax.ShapeDtypeStruct((LANES, 2 * LANES), f32),
        ),
        1 << 24,
        in_specs=[VMEM] * 6,
        out_specs=[VMEM] * 2,
    )(guess, rhs, centre, y_before, y_after, x_halos)
    outer, packed = call(
        late,
        (
            jax.ShapeDtypeStruct((2, y_cells, lane_count), f32),
            jax.ShapeDtypeStruct((columns // 2, LANES), f32),
        ),
        1 << 24,
        in_specs=[VMEM] * 4,
        out_specs=[VMEM] * 2,
    )(left, z_before, z_after, inner)
    packed = sum_over_all(packed)
    total_cells = z_cells * y_cells * x_cells * lax.axis_size(AXES)
    return call(
        functools.partial(final, total_cells),
        (
            jax.ShapeDtypeStruct(guess.shape, f32),
            jax.ShapeDtypeStruct((columns, columns), f32),
        ),
        1 << 22,
        in_specs=[VMEM] * 3,
        out_specs=[pl.BlockSpec(memory_space=pl.ANY)] * 2,
        scratch_shapes=[
            pltpu.VMEM(guess.shape, f32),
            pltpu.VMEM((columns, columns), f32),
            pltpu.SemaphoreType.DMA((z_cells + 1,)),
        ],
    )(packed, left, outer)


def solution(mesh):
    placed = (P("gz", "gy", "gx"), P("gz", "gy", "gx"), P())
    return jax.shard_map(
        local, mesh=mesh, in_specs=placed, out_specs=(P("gz", "gy", "gx"), P()), check_vma=False
    )
```

```python
import functools

import jax
import jax.numpy as jnp
from jax import lax
from jax.experimental import pallas as pl
from jax.experimental.pallas import tpu as pltpu
from jax.sharding import PartitionSpec as P


AXES = ("gz", "gy", "gx")
LANES = 128
VMEM = pl.BlockSpec(memory_space=pltpu.VMEM)
HBM = pl.BlockSpec(memory_space=pltpu.HBM)


def ring(array, axis, step):
    peers = lax.axis_size(axis)
    return lax.ppermute(array, axis, [(i, (i + step) % peers) for i in range(peers)])


def faces(array, dim, width):
    length = array.shape[dim]
    last = lax.slice_in_dim(array, length - width, length, axis=dim)
    initial = lax.slice_in_dim(array, 0, width, axis=dim)
    return last, initial


def stages_of(devices):
    bits = [1 << k for k in range(1, (devices - 1).bit_length())]
    stages = [(1,)]
    for low, high in zip(bits[0::2], bits[1::2]):
        stages.append((low | high, high | 1, low | 1))
    if len(bits) % 2:
        stages.append((bits[-1] | 1,))
    return stages


def sum_over_all(value):
    devices = lax.axis_size(AXES)
    for masks in stages_of(devices):
        got = []
        for mask in masks:
            got.append(lax.ppermute(value, AXES, [(i, i ^ mask) for i in range(devices)]))
        if len(got) == 1:
            value = value + got[0]
        else:
            far, second, first = got
            value = (value + first) + (second + far)
    return value


def half_roll(tile):
    return pltpu.roll(tile, LANES // 2, axis=1)


def split_gram(tiles):
    block = jnp.concatenate(tiles, axis=0)
    hi = block.astype(jnp.bfloat16)
    lo = (block - hi.astype(jnp.float32)).astype(jnp.bfloat16)
    both = lax.dot_general(
        hi,
        jnp.concatenate([hi, lo], axis=1),
        (((0,), (0,)), ((), ())),
        preferred_element_type=jnp.float32,
    )
    return both[:, :LANES] + 2.0 * both[:, LANES:]


def pack_gram(full):
    half, quarter = LANES // 2, LANES // 4
    low = lax.broadcasted_iota(jnp.int32, (quarter, LANES), 1) < half
    upper = jnp.where(low, full[:quarter], full[half + quarter :])
    lower = jnp.where(low, full[quarter:half], full[half : half + quarter])
    return upper + half_roll(lower)


def outer_planes(planes):
    even = lax.rem(lax.axis_index("gz"), 2) == 0
    first = jnp.where(even, planes - 1, 0)
    return first, planes - 1 - first


def inside(g_ref, b_ref, c_ref, l_ref):
    planes, rows, width = g_ref.shape
    chunks = width // LANES
    row = lax.broadcasted_iota(jnp.int32, (rows, LANES), 0)
    low = lax.broadcasted_iota(jnp.int32, (rows, LANES), 1) < LANES // 2
    centre = jnp.broadcast_to(c_ref[...], (rows, LANES))
    none = jnp.zeros((rows, LANES), jnp.float32)
    for z in range(planes):
        before, here = none, half_roll(g_ref[z, :, pl.ds(0, LANES)])
        for t in range(chunks):
            at = pl.ds(t * LANES, LANES)
            after = none
            if t + 1 < chunks:
                after = half_roll(g_ref[z, :, pl.ds((t + 1) * LANES, LANES)])
            x = g_ref[z, :, at]
            near = here + jnp.where(low, before, after)
            up = jnp.where(row == 0, 0.0, pltpu.roll(x, 1, axis=0))
            down = jnp.where(row == rows - 1, 0.0, pltpu.roll(x, rows - 1, axis=0))
            near = near + (up + down)
            if z > 0:
                near = near + g_ref[z - 1, :, at]
            if z < planes - 1:
                near = near + g_ref[z + 1, :, at]
            l_ref[z, :, at] = b_ref[z, :, at] - (centre * x - near)
            before, here = here, after


def edges(i_ref, yb_ref, ya_ref, xh_ref, l_ref, gram_ref):
    planes, rows, width = l_ref.shape
    chunks = width // LANES
    row = lax.broadcasted_iota(jnp.int32, (rows, LANES), 0)
    low = lax.broadcasted_iota(jnp.int32, (rows, LANES), 1) < LANES // 2
    gram = jnp.zeros((LANES, LANES), jnp.float32)
    for z in range(planes):
        tiles = []
        for t in range(chunks):
            at = pl.ds(t * LANES, LANES)
            add = jnp.where(row == 0, yb_ref[z, :, at], 0.0)
            add = jnp.where(row == rows - 1, ya_ref[z, :, at], add)
            value = i_ref[z, :, at] + add
            if t == 0:
                value = value + jnp.where(low, xh_ref[z], 0.0)
            if t == chunks - 1:
                value = value + jnp.where(low, 0.0, xh_ref[z])
            l_ref[z, :, at] = value
            tiles.append(value)
        if 0 < z < planes - 1:
            gram = gram + split_gram(tiles)
    gram_ref[...] = gram


def outer(which, l_ref, h_ref, g_ref, r_ref, o_ref):
    z = outer_planes(l_ref.shape[0])[which]
    tiles = []
    for t in range(l_ref.shape[2] // LANES):
        at = pl.ds(t * LANES, LANES)
        value = l_ref[z, :, at] + h_ref[0, :, at]
        r_ref[0, :, at] = value
        tiles.append(value)
    gram = g_ref[...] + split_gram(tiles)
    o_ref[...] = pack_gram(gram) if which else gram


def final(cells, p_ref, l_ref, first_ref, second_ref, n_ref, m_ref, buf, gram, sem):
    planes, rows, width = l_ref.shape
    half, quarter = LANES // 2, LANES // 4
    mean = p_ref[...] / jnp.float32(cells)
    row = lax.broadcasted_iota(jnp.int32, (quarter, LANES), 0)
    lane = lax.broadcasted_iota(jnp.int32, (quarter, LANES), 1)
    own = (lane == row) | (lane == row + half + quarter)
    diagonal = jnp.sum(jnp.where(own, mean, 0.0), axis=0, keepdims=True)
    diagonal = diagonal + half_roll(diagonal)
    scale = jnp.broadcast_to(lax.rsqrt(diagonal + 1e-06), (rows, LANES))
    first, second = outer_planes(planes)
    sources = [(z, l_ref.at[z]) for z in range(1, planes - 1)]
    sources += [(first, first_ref.at[0]), (second, second_ref.at[0])]
    copies = []
    for k, (z, source) in enumerate(sources):
        for t in range(width // LANES):
            at = pl.ds(t * LANES, LANES)
            buf[k, :, at] = source[:, at] * scale
        copies.append(pltpu.make_async_copy(buf.at[k], n_ref.at[z], sem.at[k]))
        copies[-1].start()
    square = jnp.concatenate([mean[:, :half], half_roll(mean)[:, :half]], axis=0)
    gram[...] = 0.5 * (square + square.T)
    copies.append(pltpu.make_async_copy(gram, m_ref, sem.at[planes]))
    copies[-1].start()
    for copy in copies:
        copy.wait()


def call(body, outs, cost, **kwargs):
    return pl.pallas_call(
        body,
        out_shape=outs,
        cost_estimate=pl.CostEstimate(flops=cost, bytes_accessed=1 << 20, transcendentals=0),
        compiler_params=pltpu.CompilerParams(vmem_limit_bytes=16 << 20),
        **kwargs,
    )


def pairs_along(array, offset):
    peers = lax.axis_size("gz")
    partner = {}
    for i in range(offset, peers + offset, 2):
        partner[i % peers], partner[(i + 1) % peers] = (i + 1) % peers, i % peers
    return lax.ppermute(array, "gz", sorted(partner.items()))


def local(rhs, guess, shifts):
    z_cells, y_cells, lane_count = guess.shape
    columns = shifts.shape[0]
    x_cells = lane_count // columns
    f32 = jnp.float32
    whole = jax.ShapeDtypeStruct(guess.shape, f32)
    face = jax.ShapeDtypeStruct((1, y_cells, lane_count), f32)
    square = jax.ShapeDtypeStruct((LANES, LANES), f32)
    packed = jax.ShapeDtypeStruct((columns // 2, LANES), f32)
    first, second = (
        lax.dynamic_slice_in_dim(guess, z, 1, 0) for z in outer_planes(z_cells)
    )
    first = pairs_along(first, 0)
    second = pairs_along(second, 1)
    last, initial = faces(guess, 1, 1)
    y_before = ring(last, "gy", 1)
    y_after = ring(initial, "gy", -1)
    last, initial = faces(guess, 2, columns)
    if lax.axis_size("gx") == 2:
        x_halos = ring(jnp.concatenate([last, initial], axis=2), "gx", 1)
    else:
        x_halos = jnp.concatenate(
            [ring(last, "gx", 1), ring(initial, "gx", -1)], axis=2
        )
    centre = jnp.tile(6.0 + shifts, LANES // columns)[None]
    left = call(inside, whole, 1 << 24, in_specs=[VMEM] * 3, out_specs=VMEM)(guess, rhs, centre)
    left, gram = call(
        edges,
        (whole, square),
        1 << 24,
        in_specs=[VMEM] * 4,
        out_specs=[VMEM] * 2,
        input_output_aliases={0: 0},
    )(left, y_before, y_after, x_halos)
    first, gram = call(
        functools.partial(outer, 0),
        (face, square),
        1 << 22,
        in_specs=[VMEM] * 3,
        out_specs=[VMEM] * 2,
    )(left, first, gram)
    second, total = call(
        functools.partial(outer, 1),
        (face, packed),
        1 << 22,
        in_specs=[VMEM] * 3,
        out_specs=[VMEM] * 2,
    )(left, second, gram)
    total = sum_over_all(total)
    total_cells = z_cells * y_cells * x_cells * lax.axis_size(AXES)
    return call(
        functools.partial(final, total_cells),
        (whole, jax.ShapeDtypeStruct((columns, columns), f32)),
        1 << 22,
        in_specs=[VMEM] * 4,
        out_specs=[HBM] * 2,
        scratch_shapes=[
            pltpu.VMEM(guess.shape, f32),
            pltpu.VMEM((columns, columns), f32),
            pltpu.SemaphoreType.DMA((z_cells + 1,)),
        ],
    )(total, left, first, second)


def solution(mesh):
    placed = (P("gz", "gy", "gx"), P("gz", "gy", "gx"), P())
    return jax.shard_map(
        local, mesh=mesh, in_specs=placed, out_specs=(P("gz", "gy", "gx"), P()), check_vma=False
    )
```

```python
import functools

import jax
import jax.numpy as jnp
from jax import lax
from jax.experimental import pallas as pl
from jax.experimental.pallas import tpu as pltpu
from jax.sharding import PartitionSpec as P


AXES = ("gz", "gy", "gx")
LANES = 128
VMEM = pl.BlockSpec(memory_space=pltpu.VMEM)
HBM = pl.BlockSpec(memory_space=pltpu.HBM)


def ring(array, axis, step):
    peers = lax.axis_size(axis)
    return lax.ppermute(array, axis, [(i, (i + step) % peers) for i in range(peers)])


def faces(array, dim, width):
    length = array.shape[dim]
    last = lax.slice_in_dim(array, length - width, length, axis=dim)
    initial = lax.slice_in_dim(array, 0, width, axis=dim)
    return last, initial


def stages_of(devices):
    bits = [1 << k for k in range(1, (devices - 1).bit_length())]
    stages = [(1,)]
    for low, high in zip(bits[0::2], bits[1::2]):
        stages.append((low | high, high | 1, low | 1))
    if len(bits) % 2:
        stages.append((bits[-1] | 1,))
    return stages


def sum_over_all(value):
    devices = lax.axis_size(AXES)
    for masks in stages_of(devices):
        got = []
        for mask in masks:
            got.append(lax.ppermute(value, AXES, [(i, i ^ mask) for i in range(devices)]))
        if len(got) == 1:
            value = value + got[0]
        else:
            far, second, first = got
            value = (value + first) + (second + far)
    return value


def half_roll(tile):
    return pltpu.roll(tile, LANES // 2, axis=1)


def split_gram(tiles):
    block = jnp.concatenate(tiles, axis=0)
    hi = block.astype(jnp.bfloat16)
    lo = (block - hi.astype(jnp.float32)).astype(jnp.bfloat16)
    both = lax.dot_general(
        hi,
        jnp.concatenate([hi, lo], axis=1),
        (((0,), (0,)), ((), ())),
        preferred_element_type=jnp.float32,
    )
    return both[:, :LANES] + 2.0 * both[:, LANES:]


def pack_gram(full):
    half, quarter = LANES // 2, LANES // 4
    low = lax.broadcasted_iota(jnp.int32, (quarter, LANES), 1) < half
    upper = jnp.where(low, full[:quarter], full[half + quarter :])
    lower = jnp.where(low, full[quarter:half], full[half : half + quarter])
    return upper + half_roll(lower)


def outer_planes(planes):
    same = lax.rem(lax.axis_index("gz") + lax.axis_index("gx"), 2) == 1
    first = jnp.where(same, planes - 1, 0)
    return first, planes - 1 - first


def z_faces(g_ref, first_ref, second_ref, sem):
    planes = outer_planes(g_ref.shape[0])
    copies = [
        pltpu.make_async_copy(g_ref.at[z], ref.at[0], sem.at[k])
        for k, (z, ref) in enumerate(zip(planes, (first_ref, second_ref)))
    ]
    for copy in copies:
        copy.start()
    for copy in copies:
        copy.wait()


def inside(g_ref, b_ref, c_ref, l_ref):
    planes, rows, width = g_ref.shape
    chunks = width // LANES
    row = lax.broadcasted_iota(jnp.int32, (rows, LANES), 0)
    low = lax.broadcasted_iota(jnp.int32, (rows, LANES), 1) < LANES // 2
    centre = jnp.broadcast_to(c_ref[...], (rows, LANES))
    none = jnp.zeros((rows, LANES), jnp.float32)
    for z in range(planes):
        before, here = none, half_roll(g_ref[z, :, pl.ds(0, LANES)])
        for t in range(chunks):
            at = pl.ds(t * LANES, LANES)
            after = none
            if t + 1 < chunks:
                after = half_roll(g_ref[z, :, pl.ds((t + 1) * LANES, LANES)])
            x = g_ref[z, :, at]
            near = here + jnp.where(low, before, after)
            up = jnp.where(row == 0, 0.0, pltpu.roll(x, 1, axis=0))
            down = jnp.where(row == rows - 1, 0.0, pltpu.roll(x, rows - 1, axis=0))
            near = near + (up + down)
            if z > 0:
                near = near + g_ref[z - 1, :, at]
            if z < planes - 1:
                near = near + g_ref[z + 1, :, at]
            l_ref[z, :, at] = b_ref[z, :, at] - (centre * x - near)
            before, here = here, after


def edges(i_ref, yb_ref, ya_ref, xh_ref, l_ref, gram_ref):
    planes, rows, width = l_ref.shape
    chunks = width // LANES
    row = lax.broadcasted_iota(jnp.int32, (rows, LANES), 0)
    low = lax.broadcasted_iota(jnp.int32, (rows, LANES), 1) < LANES // 2
    gram = jnp.zeros((LANES, LANES), jnp.float32)
    for z in range(planes):
        tiles = []
        for t in range(chunks):
            at = pl.ds(t * LANES, LANES)
            add = jnp.where(row == 0, yb_ref[z, :, at], 0.0)
            add = jnp.where(row == rows - 1, ya_ref[z, :, at], add)
            value = i_ref[z, :, at] + add
            if t == 0:
                value = value + jnp.where(low, xh_ref[z], 0.0)
            if t == chunks - 1:
                value = value + jnp.where(low, 0.0, xh_ref[z])
            l_ref[z, :, at] = value
            tiles.append(value)
        if 0 < z < planes - 1:
            gram = gram + split_gram(tiles)
    gram_ref[...] = gram


def outer(which, l_ref, h_ref, g_ref, r_ref, o_ref):
    z = outer_planes(l_ref.shape[0])[which]
    tiles = []
    for t in range(l_ref.shape[2] // LANES):
        at = pl.ds(t * LANES, LANES)
        value = l_ref[z, :, at] + h_ref[0, :, at]
        r_ref[0, :, at] = value
        tiles.append(value)
    gram = g_ref[...] + split_gram(tiles)
    o_ref[...] = pack_gram(gram) if which else gram


def final(cells, p_ref, l_ref, first_ref, second_ref, n_ref, m_ref, buf, gram, sem):
    planes, rows, width = l_ref.shape
    half, quarter = LANES // 2, LANES // 4
    mean = p_ref[...] / jnp.float32(cells)
    row = lax.broadcasted_iota(jnp.int32, (quarter, LANES), 0)
    lane = lax.broadcasted_iota(jnp.int32, (quarter, LANES), 1)
    own = (lane == row) | (lane == row + half + quarter)
    diagonal = jnp.sum(jnp.where(own, mean, 0.0), axis=0, keepdims=True)
    diagonal = diagonal + half_roll(diagonal)
    scale = jnp.broadcast_to(lax.rsqrt(diagonal + 1e-06), (rows, LANES))
    first, second = outer_planes(planes)
    sources = [(z, l_ref.at[z]) for z in range(1, planes - 1)]
    sources += [(first, first_ref.at[0]), (second, second_ref.at[0])]
    copies = []
    for k, (z, source) in enumerate(sources):
        for t in range(width // LANES):
            at = pl.ds(t * LANES, LANES)
            buf[k, :, at] = source[:, at] * scale
        copies.append(pltpu.make_async_copy(buf.at[k], n_ref.at[z], sem.at[k]))
        copies[-1].start()
    square = jnp.concatenate([mean[:, :half], half_roll(mean)[:, :half]], axis=0)
    gram[...] = 0.5 * (square + square.T)
    copies.append(pltpu.make_async_copy(gram, m_ref, sem.at[planes]))
    copies[-1].start()
    for copy in copies:
        copy.wait()


def call(body, outs, cost, limit=16 << 20, **kwargs):
    return pl.pallas_call(
        body,
        out_shape=outs,
        cost_estimate=pl.CostEstimate(flops=cost, bytes_accessed=1 << 20, transcendentals=0),
        compiler_params=pltpu.CompilerParams(vmem_limit_bytes=limit),
        **kwargs,
    )


def z_exchange(array, turn):
    peers, cores = lax.axis_size("gz"), lax.axis_size("gx")
    moves = []
    for z in range(peers):
        for core in range(cores):
            up = (z + core + turn) % 2 == 1
            moves.append((z * cores + core, (z + (1 if up else -1)) % peers * cores + core))
    return lax.ppermute(array, ("gz", "gx"), moves)


def local(rhs, guess, shifts):
    z_cells, y_cells, lane_count = guess.shape
    columns = shifts.shape[0]
    x_cells = lane_count // columns
    f32 = jnp.float32
    whole = jax.ShapeDtypeStruct(guess.shape, f32)
    face = jax.ShapeDtypeStruct((1, y_cells, lane_count), f32)
    square = jax.ShapeDtypeStruct((LANES, LANES), f32)
    packed = jax.ShapeDtypeStruct((columns // 2, LANES), f32)
    in_vmem = pltpu.VMEM((1, y_cells, lane_count), f32)
    first, second = call(
        z_faces,
        (in_vmem, in_vmem),
        1 << 20,
        limit=60 << 20,
        in_specs=[HBM],
        out_specs=[VMEM] * 2,
        scratch_shapes=[pltpu.SemaphoreType.DMA((2,))],
    )(guess)
    first = z_exchange(first, 0)
    second = z_exchange(second, 1)
    last, initial = faces(guess, 1, 1)
    y_before = ring(last, "gy", 1)
    y_after = ring(initial, "gy", -1)
    last, initial = faces(guess, 2, columns)
    if lax.axis_size("gx") == 2:
        x_halos = ring(jnp.concatenate([last, initial], axis=2), "gx", 1)
    else:
        x_halos = jnp.concatenate(
            [ring(last, "gx", 1), ring(initial, "gx", -1)], axis=2
        )
    centre = jnp.tile(6.0 + shifts, LANES // columns)[None]
    left = call(inside, whole, 1 << 24, in_specs=[VMEM] * 3, out_specs=VMEM)(guess, rhs, centre)
    left, gram = call(
        edges,
        (whole, square),
        1 << 24,
        in_specs=[VMEM] * 4,
        out_specs=[VMEM] * 2,
        input_output_aliases={0: 0},
    )(left, y_before, y_after, x_halos)
    first, gram = call(
        functools.partial(outer, 0),
        (face, square),
        1 << 22,
        in_specs=[VMEM] * 3,
        out_specs=[VMEM] * 2,
    )(left, first, gram)
    second, total = call(
        functools.partial(outer, 1),
        (face, packed),
        1 << 22,
        in_specs=[VMEM] * 3,
        out_specs=[VMEM] * 2,
    )(left, second, gram)
    total = sum_over_all(total)
    total_cells = z_cells * y_cells * x_cells * lax.axis_size(AXES)
    return call(
        functools.partial(final, total_cells),
        (whole, jax.ShapeDtypeStruct((columns, columns), f32)),
        1 << 22,
        in_specs=[VMEM] * 4,
        out_specs=[HBM] * 2,
        scratch_shapes=[
            pltpu.VMEM(guess.shape, f32),
            pltpu.VMEM((columns, columns), f32),
            pltpu.SemaphoreType.DMA((z_cells + 1,)),
        ],
    )(total, left, first, second)


def solution(mesh):
    placed = (P("gz", "gy", "gx"), P("gz", "gy", "gx"), P())
    return jax.shard_map(
        local, mesh=mesh, in_specs=placed, out_specs=(P("gz", "gy", "gx"), P()), check_vma=False
    )
```

```python
import functools

import jax
import jax.numpy as jnp
from jax import lax
from jax.experimental import pallas as pl
from jax.experimental.pallas import tpu as pltpu
from jax.sharding import PartitionSpec as P


AXES = ("gz", "gy", "gx")
LANES = 128
VMEM = pl.BlockSpec(memory_space=pltpu.VMEM)
HBM = pl.BlockSpec(memory_space=pltpu.HBM)


def ring(array, axis, step):
    peers = lax.axis_size(axis)
    return lax.ppermute(array, axis, [(i, (i + step) % peers) for i in range(peers)])


def faces(array, dim, width):
    length = array.shape[dim]
    last = lax.slice_in_dim(array, length - width, length, axis=dim)
    initial = lax.slice_in_dim(array, 0, width, axis=dim)
    return last, initial


def stages_of(devices):
    bits = [1 << k for k in range(1, (devices - 1).bit_length())]
    stages = [(1,)]
    for low, high in zip(bits[0::2], bits[1::2]):
        stages.append((low | high, high | 1, low | 1))
    if len(bits) % 2:
        stages.append((bits[-1] | 1,))
    return stages


def sum_over_all(value):
    devices = lax.axis_size(AXES)
    for masks in stages_of(devices):
        got = []
        for mask in masks:
            got.append(lax.ppermute(value, AXES, [(i, i ^ mask) for i in range(devices)]))
        if len(got) == 1:
            value = value + got[0]
        else:
            far, second, first = got
            value = (value + first) + (second + far)
    return value


def half_roll(tile):
    return pltpu.roll(tile, LANES // 2, axis=1)


def split_gram(tiles):
    block = jnp.concatenate(tiles, axis=0)
    hi = block.astype(jnp.bfloat16)
    lo = (block - hi.astype(jnp.float32)).astype(jnp.bfloat16)
    both = lax.dot_general(
        hi,
        jnp.concatenate([hi, lo], axis=1),
        (((0,), (0,)), ((), ())),
        preferred_element_type=jnp.float32,
    )
    return both[:, :LANES] + 2.0 * both[:, LANES:]


def pack_gram(full):
    half, quarter = LANES // 2, LANES // 4
    low = lax.broadcasted_iota(jnp.int32, (quarter, LANES), 1) < half
    upper = jnp.where(low, full[:quarter], full[half + quarter :])
    lower = jnp.where(low, full[quarter:half], full[half : half + quarter])
    return upper + half_roll(lower)


def outer_planes(planes):
    same = lax.rem(lax.axis_index("gz") + lax.axis_index("gx"), 2) == 1
    first = jnp.where(same, planes - 1, 0)
    return first, planes - 1 - first


def run_copies(pairs, sem):
    copies = [
        pltpu.make_async_copy(source, target, sem.at[k])
        for k, (source, target) in enumerate(pairs)
    ]
    for copy in copies:
        copy.start()
    for copy in copies:
        copy.wait()


def z_faces(g_ref, first_ref, second_ref, sem):
    first, second = outer_planes(g_ref.shape[0])
    run_copies(((g_ref.at[first], first_ref.at[0]), (g_ref.at[second], second_ref.at[0])), sem)


def load(g_ref, b_ref, g_out, b_out, sem):
    run_copies(((g_ref, g_out), (b_ref, b_out)), sem)


def inside(g_ref, b_ref, c_ref, l_ref):
    planes, rows, width = g_ref.shape
    chunks = width // LANES
    row = lax.broadcasted_iota(jnp.int32, (rows, LANES), 0)
    low = lax.broadcasted_iota(jnp.int32, (rows, LANES), 1) < LANES // 2
    centre = jnp.broadcast_to(c_ref[...], (rows, LANES))
    none = jnp.zeros((rows, LANES), jnp.float32)
    for z in range(planes):
        before, here = none, half_roll(g_ref[z, :, pl.ds(0, LANES)])
        for t in range(chunks):
            at = pl.ds(t * LANES, LANES)
            after = none
            if t + 1 < chunks:
                after = half_roll(g_ref[z, :, pl.ds((t + 1) * LANES, LANES)])
            x = g_ref[z, :, at]
            near = here + jnp.where(low, before, after)
            up = jnp.where(row == 0, 0.0, pltpu.roll(x, 1, axis=0))
            down = jnp.where(row == rows - 1, 0.0, pltpu.roll(x, rows - 1, axis=0))
            near = near + (up + down)
            if z > 0:
                near = near + g_ref[z - 1, :, at]
            if z < planes - 1:
                near = near + g_ref[z + 1, :, at]
            l_ref[z, :, at] = b_ref[z, :, at] - (centre * x - near)
            before, here = here, after


def edges(i_ref, yb_ref, ya_ref, xh_ref, l_ref, gram_ref):
    planes, rows, width = l_ref.shape
    chunks = width // LANES
    row = lax.broadcasted_iota(jnp.int32, (rows, LANES), 0)
    low = lax.broadcasted_iota(jnp.int32, (rows, LANES), 1) < LANES // 2
    gram = jnp.zeros((LANES, LANES), jnp.float32)
    for z in range(planes):
        tiles = []
        for t in range(chunks):
            at = pl.ds(t * LANES, LANES)
            add = jnp.where(row == 0, yb_ref[z, :, at], 0.0)
            add = jnp.where(row == rows - 1, ya_ref[z, :, at], add)
            value = i_ref[z, :, at] + add
            if t == 0:
                value = value + jnp.where(low, xh_ref[z], 0.0)
            if t == chunks - 1:
                value = value + jnp.where(low, 0.0, xh_ref[z])
            l_ref[z, :, at] = value
            tiles.append(value)
        if 0 < z < planes - 1:
            gram = gram + split_gram(tiles)
    gram_ref[...] = gram


def outer(which, l_ref, h_ref, g_ref, r_ref, o_ref):
    z = outer_planes(l_ref.shape[0])[which]
    tiles = []
    for t in range(l_ref.shape[2] // LANES):
        at = pl.ds(t * LANES, LANES)
        value = l_ref[z, :, at] + h_ref[0, :, at]
        r_ref[0, :, at] = value
        tiles.append(value)
    gram = g_ref[...] + split_gram(tiles)
    o_ref[...] = pack_gram(gram) if which else gram


def final(cells, p_ref, l_ref, first_ref, second_ref, n_ref, m_ref, buf, gram, sem):
    planes, rows, width = l_ref.shape
    half, quarter = LANES // 2, LANES // 4
    mean = p_ref[...] / jnp.float32(cells)
    row = lax.broadcasted_iota(jnp.int32, (quarter, LANES), 0)
    lane = lax.broadcasted_iota(jnp.int32, (quarter, LANES), 1)
    own = (lane == row) | (lane == row + half + quarter)
    diagonal = jnp.sum(jnp.where(own, mean, 0.0), axis=0, keepdims=True)
    diagonal = diagonal + half_roll(diagonal)
    scale = jnp.broadcast_to(lax.rsqrt(diagonal + 1e-06), (rows, LANES))
    first, second = outer_planes(planes)
    sources = [(z, l_ref.at[z]) for z in range(1, planes - 1)]
    sources += [(first, first_ref.at[0]), (second, second_ref.at[0])]
    copies = []
    for k, (z, source) in enumerate(sources):
        for t in range(width // LANES):
            at = pl.ds(t * LANES, LANES)
            buf[k, :, at] = source[:, at] * scale
        copies.append(pltpu.make_async_copy(buf.at[k], n_ref.at[z], sem.at[k]))
        copies[-1].start()
    square = jnp.concatenate([mean[:, :half], half_roll(mean)[:, :half]], axis=0)
    gram[...] = 0.5 * (square + square.T)
    copies.append(pltpu.make_async_copy(gram, m_ref, sem.at[planes]))
    copies[-1].start()
    for copy in copies:
        copy.wait()


def call(body, outs, cost, limit=16 << 20, **kwargs):
    return pl.pallas_call(
        body,
        out_shape=outs,
        cost_estimate=pl.CostEstimate(flops=cost, bytes_accessed=1 << 20, transcendentals=0),
        compiler_params=pltpu.CompilerParams(vmem_limit_bytes=limit),
        **kwargs,
    )


def z_exchange(array, turn):
    peers, cores = lax.axis_size("gz"), lax.axis_size("gx")
    moves = []
    for z in range(peers):
        for core in range(cores):
            up = (z + core + turn) % 2 == 1
            moves.append((z * cores + core, (z + (1 if up else -1)) % peers * cores + core))
    return lax.ppermute(array, ("gz", "gx"), moves)


def local(rhs, guess, shifts):
    z_cells, y_cells, lane_count = guess.shape
    columns = shifts.shape[0]
    x_cells = lane_count // columns
    f32 = jnp.float32
    whole = jax.ShapeDtypeStruct(guess.shape, f32)
    face = jax.ShapeDtypeStruct((1, y_cells, lane_count), f32)
    square = jax.ShapeDtypeStruct((LANES, LANES), f32)
    packed = jax.ShapeDtypeStruct((columns // 2, LANES), f32)
    in_vmem = pltpu.VMEM((1, y_cells, lane_count), f32)
    first, second = call(
        z_faces,
        (in_vmem, in_vmem),
        1 << 20,
        limit=60 << 20,
        in_specs=[HBM],
        out_specs=[VMEM] * 2,
        scratch_shapes=[pltpu.SemaphoreType.DMA((2,))],
    )(guess)
    first = z_exchange(first, 0)
    second = z_exchange(second, 1)
    in_vmem = pltpu.VMEM(guess.shape, f32)
    guess, rhs = call(
        load,
        (in_vmem, in_vmem),
        1 << 20,
        limit=60 << 20,
        in_specs=[HBM] * 2,
        out_specs=[VMEM] * 2,
        scratch_shapes=[pltpu.SemaphoreType.DMA((2,))],
    )(guess, rhs)
    last, initial = faces(guess, 1, 1)
    y_before = ring(last, "gy", 1)
    y_after = ring(initial, "gy", -1)
    last, initial = faces(guess, 2, columns)
    if lax.axis_size("gx") == 2:
        x_halos = ring(jnp.concatenate([last, initial], axis=2), "gx", 1)
    else:
        x_halos = jnp.concatenate(
            [ring(last, "gx", 1), ring(initial, "gx", -1)], axis=2
        )
    centre = jnp.tile(6.0 + shifts, LANES // columns)[None]
    left = call(inside, whole, 1 << 24, in_specs=[VMEM] * 3, out_specs=VMEM)(guess, rhs, centre)
    left, gram = call(
        edges,
        (whole, square),
        1 << 24,
        in_specs=[VMEM] * 4,
        out_specs=[VMEM] * 2,
        input_output_aliases={0: 0},
    )(left, y_before, y_after, x_halos)
    first, gram = call(
        functools.partial(outer, 0),
        (face, square),
        1 << 22,
        in_specs=[VMEM] * 3,
        out_specs=[VMEM] * 2,
    )(left, first, gram)
    second, total = call(
        functools.partial(outer, 1),
        (face, packed),
        1 << 22,
        in_specs=[VMEM] * 3,
        out_specs=[VMEM] * 2,
    )(left, second, gram)
    total = sum_over_all(total)
    total_cells = z_cells * y_cells * x_cells * lax.axis_size(AXES)
    return call(
        functools.partial(final, total_cells),
        (whole, jax.ShapeDtypeStruct((columns, columns), f32)),
        1 << 22,
        in_specs=[VMEM] * 4,
        out_specs=[HBM] * 2,
        scratch_shapes=[
            pltpu.VMEM(guess.shape, f32),
            pltpu.VMEM((columns, columns), f32),
            pltpu.SemaphoreType.DMA((z_cells + 1,)),
        ],
    )(total, left, first, second)


def solution(mesh):
    placed = (P("gz", "gy", "gx"), P("gz", "gy", "gx"), P())
    return jax.shard_map(
        local, mesh=mesh, in_specs=placed, out_specs=(P("gz", "gy", "gx"), P()), check_vma=False
    )
```

```python
import functools

import jax
import jax.numpy as jnp
from jax import lax
from jax.experimental import pallas as pl
from jax.experimental.pallas import tpu as pltpu
from jax.sharding import PartitionSpec as P


AXES = ("gz", "gy", "gx")
LANES = 128
HOLD = 800
VMEM = pl.BlockSpec(memory_space=pltpu.VMEM)
HBM = pl.BlockSpec(memory_space=pltpu.HBM)


def ring(array, axis, step):
    peers = lax.axis_size(axis)
    return lax.ppermute(array, axis, [(i, (i + step) % peers) for i in range(peers)])


def faces(array, dim, width):
    length = array.shape[dim]
    last = lax.slice_in_dim(array, length - width, length, axis=dim)
    initial = lax.slice_in_dim(array, 0, width, axis=dim)
    return last, initial


def stages_of(devices):
    bits = [1 << k for k in range(1, (devices - 1).bit_length())]
    stages = [(1,)]
    for low, high in zip(bits[0::2], bits[1::2]):
        stages.append((low | high, high, low))
    if len(bits) % 2:
        stages.append((bits[-1],))
    return stages[::-1]


def sum_over_all(value):
    devices = lax.axis_size(AXES)
    for masks in stages_of(devices):
        got = []
        for mask in masks:
            got.append(lax.ppermute(value, AXES, [(i, i ^ mask) for i in range(devices)]))
        if len(got) == 1:
            value = value + got[0]
        else:
            far, second, first = got
            value = (value + first) + (second + far)
    return value


def half_roll(tile):
    return pltpu.roll(tile, LANES // 2, axis=1)


def split_gram(tiles):
    block = jnp.concatenate(tiles, axis=0)
    hi = block.astype(jnp.bfloat16)
    lo = (block - hi.astype(jnp.float32)).astype(jnp.bfloat16)
    both = lax.dot_general(
        hi,
        jnp.concatenate([hi, lo], axis=1),
        (((0,), (0,)), ((), ())),
        preferred_element_type=jnp.float32,
    )
    return both[:, :LANES] + 2.0 * both[:, LANES:]


def pack_gram(full):
    half, quarter = LANES // 2, LANES // 4
    low = lax.broadcasted_iota(jnp.int32, (quarter, LANES), 1) < half
    upper = jnp.where(low, full[:quarter], full[half + quarter :])
    lower = jnp.where(low, full[quarter:half], full[half : half + quarter])
    return upper + half_roll(lower)


def outer_planes(planes):
    even = lax.rem(lax.axis_index("gz"), 2) == 0
    first = jnp.where(even, planes - 1, 0)
    return first, planes - 1 - first


def run_copies(pairs, sem):
    copies = [
        pltpu.make_async_copy(source, target, sem.at[k])
        for k, (source, target) in enumerate(pairs)
    ]
    for copy in copies:
        copy.start()
    for copy in copies:
        copy.wait()


def z_faces(g_ref, first_ref, second_ref, sem, spent):
    first, second = outer_planes(g_ref.shape[0])
    odd = lax.rem(lax.axis_index("gx"), 2)
    spent[0] = lax.fori_loop(0, odd * HOLD, lambda _, x: x * 1664525 + 1013904223, odd)
    run_copies(((g_ref.at[first], first_ref.at[0]), (g_ref.at[second], second_ref.at[0])), sem)


def load(g_ref, b_ref, g_out, b_out, sem):
    run_copies(((g_ref, g_out), (b_ref, b_out)), sem)


def inside(g_ref, b_ref, c_ref, l_ref):
    planes, rows, width = g_ref.shape
    chunks = width // LANES
    row = lax.broadcasted_iota(jnp.int32, (rows, LANES), 0)
    low = lax.broadcasted_iota(jnp.int32, (rows, LANES), 1) < LANES // 2
    centre = jnp.broadcast_to(c_ref[...], (rows, LANES))
    none = jnp.zeros((rows, LANES), jnp.float32)
    for z in range(planes):
        before, here = none, half_roll(g_ref[z, :, pl.ds(0, LANES)])
        for t in range(chunks):
            at = pl.ds(t * LANES, LANES)
            after = none
            if t + 1 < chunks:
                after = half_roll(g_ref[z, :, pl.ds((t + 1) * LANES, LANES)])
            x = g_ref[z, :, at]
            near = here + jnp.where(low, before, after)
            up = jnp.where(row == 0, 0.0, pltpu.roll(x, 1, axis=0))
            down = jnp.where(row == rows - 1, 0.0, pltpu.roll(x, rows - 1, axis=0))
            near = near + (up + down)
            if z > 0:
                near = near + g_ref[z - 1, :, at]
            if z < planes - 1:
                near = near + g_ref[z + 1, :, at]
            l_ref[z, :, at] = b_ref[z, :, at] - (centre * x - near)
            before, here = here, after


def edges(i_ref, yb_ref, ya_ref, xh_ref, l_ref, gram_ref):
    planes, rows, width = l_ref.shape
    chunks = width // LANES
    row = lax.broadcasted_iota(jnp.int32, (rows, LANES), 0)
    low = lax.broadcasted_iota(jnp.int32, (rows, LANES), 1) < LANES // 2
    gram = jnp.zeros((LANES, LANES), jnp.float32)
    for z in range(planes):
        tiles = []
        for t in range(chunks):
            at = pl.ds(t * LANES, LANES)
            add = jnp.where(row == 0, yb_ref[z, :, at], 0.0)
            add = jnp.where(row == rows - 1, ya_ref[z, :, at], add)
            value = i_ref[z, :, at] + add
            if t == 0:
                value = value + jnp.where(low, xh_ref[z], 0.0)
            if t == chunks - 1:
                value = value + jnp.where(low, 0.0, xh_ref[z])
            l_ref[z, :, at] = value
            tiles.append(value)
        if 0 < z < planes - 1:
            gram = gram + split_gram(tiles)
    gram_ref[...] = gram


def outer(which, l_ref, h_ref, g_ref, r_ref, o_ref):
    z = outer_planes(l_ref.shape[0])[which]
    tiles = []
    for t in range(l_ref.shape[2] // LANES):
        at = pl.ds(t * LANES, LANES)
        value = l_ref[z, :, at] + h_ref[0, :, at]
        r_ref[0, :, at] = value
        tiles.append(value)
    gram = g_ref[...] + split_gram(tiles)
    o_ref[...] = pack_gram(gram) if which else gram


def final(cells, p_ref, l_ref, first_ref, second_ref, n_ref, m_ref, buf, gram, sem):
    planes, rows, width = l_ref.shape
    half, quarter = LANES // 2, LANES // 4
    mean = p_ref[...] / jnp.float32(cells)
    row = lax.broadcasted_iota(jnp.int32, (quarter, LANES), 0)
    lane = lax.broadcasted_iota(jnp.int32, (quarter, LANES), 1)
    own = (lane == row) | (lane == row + half + quarter)
    diagonal = jnp.sum(jnp.where(own, mean, 0.0), axis=0, keepdims=True)
    diagonal = diagonal + half_roll(diagonal)
    scale = jnp.broadcast_to(lax.rsqrt(diagonal + 1e-06), (rows, LANES))
    first, second = outer_planes(planes)
    sources = [(z, l_ref.at[z]) for z in range(1, planes - 1)]
    sources += [(first, first_ref.at[0]), (second, second_ref.at[0])]
    copies = []
    for k, (z, source) in enumerate(sources):
        for t in range(width // LANES):
            at = pl.ds(t * LANES, LANES)
            buf[k, :, at] = source[:, at] * scale
        copies.append(pltpu.make_async_copy(buf.at[k], n_ref.at[z], sem.at[k]))
        copies[-1].start()
    square = jnp.concatenate([mean[:, :half], half_roll(mean)[:, :half]], axis=0)
    gram[...] = 0.5 * (square + square.T)
    copies.append(pltpu.make_async_copy(gram, m_ref, sem.at[planes]))
    copies[-1].start()
    for copy in copies:
        copy.wait()


def call(body, outs, cost, limit=16 << 20, **kwargs):
    return pl.pallas_call(
        body,
        out_shape=outs,
        cost_estimate=pl.CostEstimate(flops=cost, bytes_accessed=1 << 20, transcendentals=0),
        compiler_params=pltpu.CompilerParams(vmem_limit_bytes=limit),
        **kwargs,
    )


def z_exchange(array, turn):
    peers = lax.axis_size("gz")
    moves = [(z, (z + (1 if (z + turn) % 2 == 0 else -1)) % peers) for z in range(peers)]
    return lax.ppermute(array, "gz", moves)


def local(rhs, guess, shifts):
    z_cells, y_cells, lane_count = guess.shape
    columns = shifts.shape[0]
    x_cells = lane_count // columns
    f32 = jnp.float32
    whole = jax.ShapeDtypeStruct(guess.shape, f32)
    face = jax.ShapeDtypeStruct((1, y_cells, lane_count), f32)
    square = jax.ShapeDtypeStruct((LANES, LANES), f32)
    packed = jax.ShapeDtypeStruct((columns // 2, LANES), f32)
    in_vmem = pltpu.VMEM((1, y_cells, lane_count), f32)
    first, second = call(
        z_faces,
        (in_vmem, in_vmem),
        1 << 20,
        limit=60 << 20,
        in_specs=[HBM],
        out_specs=[VMEM] * 2,
        scratch_shapes=[pltpu.SemaphoreType.DMA((2,)), pltpu.SMEM((1,), jnp.int32)],
    )(guess)
    first = z_exchange(first, 0)
    second = z_exchange(second, 1)
    in_vmem = pltpu.VMEM(guess.shape, f32)
    guess, rhs = call(
        load,
        (in_vmem, in_vmem),
        1 << 20,
        limit=60 << 20,
        in_specs=[HBM] * 2,
        out_specs=[VMEM] * 2,
        scratch_shapes=[pltpu.SemaphoreType.DMA((2,))],
    )(guess, rhs)
    last, initial = faces(guess, 1, 1)
    y_before = ring(last, "gy", 1)
    y_after = ring(initial, "gy", -1)
    last, initial = faces(guess, 2, columns)
    if lax.axis_size("gx") == 2:
        x_halos = ring(jnp.concatenate([last, initial], axis=2), "gx", 1)
    else:
        x_halos = jnp.concatenate(
            [ring(last, "gx", 1), ring(initial, "gx", -1)], axis=2
        )
    centre = jnp.tile(6.0 + shifts, LANES // columns)[None]
    left = call(inside, whole, 1 << 24, in_specs=[VMEM] * 3, out_specs=VMEM)(guess, rhs, centre)
    left, gram = call(
        edges,
        (whole, square),
        1 << 24,
        in_specs=[VMEM] * 4,
        out_specs=[VMEM] * 2,
        input_output_aliases={0: 0},
    )(left, y_before, y_after, x_halos)
    first, gram = call(
        functools.partial(outer, 0),
        (face, square),
        1 << 22,
        in_specs=[VMEM] * 3,
        out_specs=[VMEM] * 2,
    )(left, first, gram)
    second, total = call(
        functools.partial(outer, 1),
        (face, packed),
        1 << 22,
        in_specs=[VMEM] * 3,
        out_specs=[VMEM] * 2,
    )(left, second, gram)
    total = sum_over_all(total)
    total_cells = z_cells * y_cells * x_cells * lax.axis_size(AXES)
    return call(
        functools.partial(final, total_cells),
        (whole, jax.ShapeDtypeStruct((columns, columns), f32)),
        1 << 22,
        in_specs=[VMEM] * 4,
        out_specs=[HBM] * 2,
        scratch_shapes=[
            pltpu.VMEM(guess.shape, f32),
            pltpu.VMEM((columns, columns), f32),
            pltpu.SemaphoreType.DMA((z_cells + 1,)),
        ],
    )(total, left, first, second)


def solution(mesh):
    placed = (P("gz", "gy", "gx"), P("gz", "gy", "gx"), P())
    return jax.shard_map(
        local, mesh=mesh, in_specs=placed, out_specs=(P("gz", "gy", "gx"), P()), check_vma=False
    )
```

```python
import functools

import jax
import jax.numpy as jnp
from jax import lax
from jax.experimental import pallas as pl
from jax.experimental.pallas import tpu as pltpu
from jax.sharding import PartitionSpec as P


AXES = ("gz", "gy", "gx")
LANES = 128
HOLD = 950
VMEM = pl.BlockSpec(memory_space=pltpu.VMEM)
HBM = pl.BlockSpec(memory_space=pltpu.HBM)


def ring(array, axis, step):
    peers = lax.axis_size(axis)
    return lax.ppermute(array, axis, [(i, (i + step) % peers) for i in range(peers)])


def faces(array, dim, width):
    length = array.shape[dim]
    last = lax.slice_in_dim(array, length - width, length, axis=dim)
    initial = lax.slice_in_dim(array, 0, width, axis=dim)
    return last, initial


def stages_of(devices):
    bits = [1 << k for k in range(1, (devices - 1).bit_length())]
    stages = [(1,)]
    for low, high in zip(bits[0::2], bits[1::2]):
        stages.append((low | high, high, low))
    if len(bits) % 2:
        stages.append((bits[-1],))
    return stages[::-1]


def sum_over_all(value):
    devices = lax.axis_size(AXES)
    for masks in stages_of(devices):
        got = []
        for mask in masks:
            got.append(lax.ppermute(value, AXES, [(i, i ^ mask) for i in range(devices)]))
        if len(got) == 1:
            value = value + got[0]
        else:
            far, second, first = got
            value = (value + first) + (second + far)
    return value


def half_roll(tile):
    return pltpu.roll(tile, LANES // 2, axis=1)


def split_gram(tiles):
    block = jnp.concatenate(tiles, axis=0)
    hi = block.astype(jnp.bfloat16)
    lo = (block - hi.astype(jnp.float32)).astype(jnp.bfloat16)
    both = lax.dot_general(
        hi,
        jnp.concatenate([hi, lo], axis=1),
        (((0,), (0,)), ((), ())),
        preferred_element_type=jnp.float32,
    )
    return both[:, :LANES] + 2.0 * both[:, LANES:]


def pack_gram(full):
    half, quarter = LANES // 2, LANES // 4
    low = lax.broadcasted_iota(jnp.int32, (quarter, LANES), 1) < half
    upper = jnp.where(low, full[:quarter], full[half + quarter :])
    lower = jnp.where(low, full[quarter:half], full[half : half + quarter])
    return upper + half_roll(lower)


def outer_planes(planes):
    even = lax.rem(lax.axis_index("gz"), 2) == 0
    first = jnp.where(even, planes - 1, 0)
    return first, planes - 1 - first


def is_odd_core():
    return lax.rem(lax.axis_index("gx"), 2) == 1


def run_copies(pairs, sem):
    copies = [
        pltpu.make_async_copy(source, target, sem.at[k])
        for k, (source, target) in enumerate(pairs)
    ]
    for copy in copies:
        copy.start()
    for copy in copies:
        copy.wait()


def inside(g_ref, b_ref, s_ref, l_ref):
    planes, rows, width = g_ref.shape
    chunks = width // LANES
    row = lax.broadcasted_iota(jnp.int32, (rows, LANES), 0)
    low = lax.broadcasted_iota(jnp.int32, (rows, LANES), 1) < LANES // 2
    centre = 6.0 + s_ref[...]
    centre = jnp.broadcast_to(jnp.concatenate([centre, centre], axis=1), (rows, LANES))
    none = jnp.zeros((rows, LANES), jnp.float32)
    for z in range(planes):
        before, here = none, half_roll(g_ref[z, :, pl.ds(0, LANES)])
        for t in range(chunks):
            at = pl.ds(t * LANES, LANES)
            after = none
            if t + 1 < chunks:
                after = half_roll(g_ref[z, :, pl.ds((t + 1) * LANES, LANES)])
            x = g_ref[z, :, at]
            near = here + jnp.where(low, before, after)
            up = jnp.where(row == 0, 0.0, pltpu.roll(x, 1, axis=0))
            down = jnp.where(row == rows - 1, 0.0, pltpu.roll(x, rows - 1, axis=0))
            near = near + (up + down)
            if z > 0:
                near = near + g_ref[z - 1, :, at]
            if z < planes - 1:
                near = near + g_ref[z + 1, :, at]
            l_ref[z, :, at] = b_ref[z, :, at] - (centre * x - near)
            before, here = here, after


def head(g_ref, b_ref, s_ref, first_ref, second_ref, g_out, l_out, b_buf, s_buf, spent, sem):
    first, second = outer_planes(g_ref.shape[0])
    faces = ((g_ref.at[first], first_ref.at[0]), (g_ref.at[second], second_ref.at[0]))
    odd = is_odd_core()

    @pl.when(odd)
    def _():
        run_copies(faces + ((g_ref, g_out), (b_ref, b_buf), (s_ref, s_buf)), sem)
        inside(g_out, b_buf, s_buf, l_out)
        spent[0] = lax.fori_loop(0, HOLD, lambda _, x: x * 1664525 + 1013904223, 1)

    @pl.when(jnp.logical_not(odd))
    def _():
        run_copies(faces, sem)


def rest(g_ref, b_ref, s_ref, g_in, l_in, g_out, l_out, b_buf, s_buf, sem):
    odd = is_odd_core()

    @pl.when(odd)
    def _():
        g_out[...] = g_in[...]
        l_out[...] = l_in[...]

    @pl.when(jnp.logical_not(odd))
    def _():
        run_copies(((g_ref, g_out), (b_ref, b_buf), (s_ref, s_buf)), sem)
        inside(g_out, b_buf, s_buf, l_out)


def edges(i_ref, yb_ref, ya_ref, xh_ref, l_ref, gram_ref):
    planes, rows, width = l_ref.shape
    chunks = width // LANES
    row = lax.broadcasted_iota(jnp.int32, (rows, LANES), 0)
    low = lax.broadcasted_iota(jnp.int32, (rows, LANES), 1) < LANES // 2
    gram = jnp.zeros((LANES, LANES), jnp.float32)
    for z in range(planes):
        tiles = []
        for t in range(chunks):
            at = pl.ds(t * LANES, LANES)
            add = jnp.where(row == 0, yb_ref[z, :, at], 0.0)
            add = jnp.where(row == rows - 1, ya_ref[z, :, at], add)
            value = i_ref[z, :, at] + add
            if t == 0:
                value = value + jnp.where(low, xh_ref[z], 0.0)
            if t == chunks - 1:
                value = value + jnp.where(low, 0.0, xh_ref[z])
            l_ref[z, :, at] = value
            tiles.append(value)
        if 0 < z < planes - 1:
            gram = gram + split_gram(tiles)
    gram_ref[...] = gram


def outer(which, l_ref, h_ref, g_ref, r_ref, o_ref):
    z = outer_planes(l_ref.shape[0])[which]
    tiles = []
    for t in range(l_ref.shape[2] // LANES):
        at = pl.ds(t * LANES, LANES)
        value = l_ref[z, :, at] + h_ref[0, :, at]
        r_ref[0, :, at] = value
        tiles.append(value)
    gram = g_ref[...] + split_gram(tiles)
    o_ref[...] = pack_gram(gram) if which else gram


def final(cells, p_ref, l_ref, first_ref, second_ref, n_ref, m_ref, buf, gram, sem):
    planes, rows, width = l_ref.shape
    half, quarter = LANES // 2, LANES // 4
    mean = p_ref[...] / jnp.float32(cells)
    row = lax.broadcasted_iota(jnp.int32, (quarter, LANES), 0)
    lane = lax.broadcasted_iota(jnp.int32, (quarter, LANES), 1)
    own = (lane == row) | (lane == row + half + quarter)
    diagonal = jnp.sum(jnp.where(own, mean, 0.0), axis=0, keepdims=True)
    diagonal = diagonal + half_roll(diagonal)
    scale = jnp.broadcast_to(lax.rsqrt(diagonal + 1e-06), (rows, LANES))
    first, second = outer_planes(planes)
    sources = [(z, l_ref.at[z]) for z in range(1, planes - 1)]
    sources += [(first, first_ref.at[0]), (second, second_ref.at[0])]
    copies = []
    for k, (z, source) in enumerate(sources):
        for t in range(width // LANES):
            at = pl.ds(t * LANES, LANES)
            buf[k, :, at] = source[:, at] * scale
        copies.append(pltpu.make_async_copy(buf.at[k], n_ref.at[z], sem.at[k]))
        copies[-1].start()
    square = jnp.concatenate([mean[:, :half], half_roll(mean)[:, :half]], axis=0)
    gram[...] = 0.5 * (square + square.T)
    copies.append(pltpu.make_async_copy(gram, m_ref, sem.at[planes]))
    copies[-1].start()
    for copy in copies:
        copy.wait()


def call(body, outs, cost, limit=16 << 20, **kwargs):
    return pl.pallas_call(
        body,
        out_shape=outs,
        cost_estimate=pl.CostEstimate(flops=cost, bytes_accessed=1 << 20, transcendentals=0),
        compiler_params=pltpu.CompilerParams(vmem_limit_bytes=limit),
        **kwargs,
    )


def z_exchange(array, turn):
    peers = lax.axis_size("gz")
    moves = [(z, (z + (1 if (z + turn) % 2 == 0 else -1)) % peers) for z in range(peers)]
    return lax.ppermute(array, "gz", moves)


def local(rhs, guess, shifts):
    z_cells, y_cells, lane_count = guess.shape
    columns = shifts.shape[0]
    x_cells = lane_count // columns
    f32 = jnp.float32
    whole = jax.ShapeDtypeStruct(guess.shape, f32)
    face = jax.ShapeDtypeStruct((1, y_cells, lane_count), f32)
    square = jax.ShapeDtypeStruct((LANES, LANES), f32)
    packed = jax.ShapeDtypeStruct((columns // 2, LANES), f32)
    face_in_vmem = pltpu.VMEM((1, y_cells, lane_count), f32)
    whole_in_vmem = pltpu.VMEM(guess.shape, f32)
    small = shifts[None]
    scratch = [whole_in_vmem, pltpu.VMEM((1, columns), f32)]
    first, second, held, left = call(
        head,
        (face_in_vmem,) * 2 + (whole_in_vmem,) * 2,
        1 << 20,
        limit=60 << 20,
        in_specs=[HBM] * 3,
        out_specs=[VMEM] * 4,
        scratch_shapes=scratch
        + [pltpu.SMEM((1,), jnp.int32), pltpu.SemaphoreType.DMA((5,))],
    )(guess, rhs, small)
    first = z_exchange(first, 0)
    second = z_exchange(second, 1)
    guess, left = call(
        rest,
        (whole_in_vmem,) * 2,
        1 << 20,
        limit=60 << 20,
        in_specs=[HBM] * 3 + [VMEM] * 2,
        out_specs=[VMEM] * 2,
        scratch_shapes=scratch + [pltpu.SemaphoreType.DMA((3,))],
        input_output_aliases={3: 0, 4: 1},
    )(guess, rhs, small, held, left)
    last, initial = faces(guess, 1, 1)
    y_before = ring(last, "gy", 1)
    y_after = ring(initial, "gy", -1)
    last, initial = faces(guess, 2, columns)
    if lax.axis_size("gx") == 2:
        x_halos = ring(jnp.concatenate([last, initial], axis=2), "gx", 1)
    else:
        x_halos = jnp.concatenate(
            [ring(last, "gx", 1), ring(initial, "gx", -1)], axis=2
        )
    left, gram = call(
        edges,
        (whole, square),
        1 << 24,
        in_specs=[VMEM] * 4,
        out_specs=[VMEM] * 2,
        input_output_aliases={0: 0},
    )(left, y_before, y_after, x_halos)
    first, gram = call(
        functools.partial(outer, 0),
        (face, square),
        1 << 22,
        in_specs=[VMEM] * 3,
        out_specs=[VMEM] * 2,
    )(left, first, gram)
    second, total = call(
        functools.partial(outer, 1),
        (face, packed),
        1 << 22,
        in_specs=[VMEM] * 3,
        out_specs=[VMEM] * 2,
    )(left, second, gram)
    total = sum_over_all(total)
    total_cells = z_cells * y_cells * x_cells * lax.axis_size(AXES)
    return call(
        functools.partial(final, total_cells),
        (whole, jax.ShapeDtypeStruct((columns, columns), f32)),
        1 << 22,
        in_specs=[VMEM] * 4,
        out_specs=[HBM] * 2,
        scratch_shapes=[
            pltpu.VMEM(guess.shape, f32),
            pltpu.VMEM((columns, columns), f32),
            pltpu.SemaphoreType.DMA((z_cells + 1,)),
        ],
    )(total, left, first, second)


def solution(mesh):
    placed = (P("gz", "gy", "gx"), P("gz", "gy", "gx"), P())
    return jax.shard_map(
        local, mesh=mesh, in_specs=placed, out_specs=(P("gz", "gy", "gx"), P()), check_vma=False
    )
```

```python
import functools

import jax
import jax.numpy as jnp
from jax import lax
from jax.experimental import pallas as pl
from jax.experimental.pallas import tpu as pltpu
from jax.sharding import PartitionSpec as P


AXES = ("gz", "gy", "gx")
LANES = 128
HOLD = 800
VMEM = pl.BlockSpec(memory_space=pltpu.VMEM)
HBM = pl.BlockSpec(memory_space=pltpu.HBM)


def ring(array, axis, step):
    peers = lax.axis_size(axis)
    return lax.ppermute(array, axis, [(i, (i + step) % peers) for i in range(peers)])


def faces(array, dim, width):
    length = array.shape[dim]
    last = lax.slice_in_dim(array, length - width, length, axis=dim)
    initial = lax.slice_in_dim(array, 0, width, axis=dim)
    return last, initial


def stages_of(devices):
    bits = [1 << k for k in range(1, (devices - 1).bit_length())]
    triples = [(low | high, high, low) for low, high in zip(bits[0::2], bits[1::2])]
    single = [(bits[-1],)] * (len(bits) % 2)
    return list(zip(triples + single + [(1,)], triples[::-1] + single + [(1,)]))


def sum_over_all(value):
    devices = lax.axis_size(AXES)
    for odd, even in stages_of(devices):
        got = []
        for k in range(len(odd)):
            moves = [(i, i ^ (odd if i % 2 else even)[k]) for i in range(devices)]
            got.append(lax.ppermute(value, AXES, moves))
        if len(got) == 1:
            value = value + got[0]
        else:
            far, second, first = got
            value = (value + first) + (second + far)
    return value


def half_roll(tile):
    return pltpu.roll(tile, LANES // 2, axis=1)


def split_gram(tiles):
    block = jnp.concatenate(tiles, axis=0)
    hi = block.astype(jnp.bfloat16)
    lo = (block - hi.astype(jnp.float32)).astype(jnp.bfloat16)
    both = lax.dot_general(
        hi,
        jnp.concatenate([hi, lo], axis=1),
        (((0,), (0,)), ((), ())),
        preferred_element_type=jnp.float32,
    )
    return both[:, :LANES] + 2.0 * both[:, LANES:]


def pack_gram(full):
    half, quarter = LANES // 2, LANES // 4
    low = lax.broadcasted_iota(jnp.int32, (quarter, LANES), 1) < half
    upper = jnp.where(low, full[:quarter], full[half + quarter :])
    lower = jnp.where(low, full[quarter:half], full[half : half + quarter])
    return upper + half_roll(lower)


def outer_planes(planes):
    even = lax.rem(lax.axis_index("gz"), 2) == 0
    first = jnp.where(even, planes - 1, 0)
    return first, planes - 1 - first


def run_copies(pairs, sem):
    copies = [
        pltpu.make_async_copy(source, target, sem.at[k])
        for k, (source, target) in enumerate(pairs)
    ]
    for copy in copies:
        copy.start()
    for copy in copies:
        copy.wait()


def z_faces(g_ref, first_ref, second_ref, sem, spent):
    first, second = outer_planes(g_ref.shape[0])
    odd = lax.rem(lax.axis_index("gx"), 2)
    spent[0] = lax.fori_loop(0, odd * HOLD, lambda _, x: x * 1664525 + 1013904223, odd)
    run_copies(((g_ref.at[first], first_ref.at[0]), (g_ref.at[second], second_ref.at[0])), sem)


def load(g_ref, b_ref, g_out, b_out, sem):
    run_copies(((g_ref, g_out), (b_ref, b_out)), sem)


def inside(g_ref, b_ref, c_ref, l_ref):
    planes, rows, width = g_ref.shape
    chunks = width // LANES
    row = lax.broadcasted_iota(jnp.int32, (rows, LANES), 0)
    low = lax.broadcasted_iota(jnp.int32, (rows, LANES), 1) < LANES // 2
    centre = jnp.broadcast_to(c_ref[...], (rows, LANES))
    none = jnp.zeros((rows, LANES), jnp.float32)
    for z in range(planes):
        before, here = none, half_roll(g_ref[z, :, pl.ds(0, LANES)])
        for t in range(chunks):
            at = pl.ds(t * LANES, LANES)
            after = none
            if t + 1 < chunks:
                after = half_roll(g_ref[z, :, pl.ds((t + 1) * LANES, LANES)])
            x = g_ref[z, :, at]
            near = here + jnp.where(low, before, after)
            up = jnp.where(row == 0, 0.0, pltpu.roll(x, 1, axis=0))
            down = jnp.where(row == rows - 1, 0.0, pltpu.roll(x, rows - 1, axis=0))
            near = near + (up + down)
            if z > 0:
                near = near + g_ref[z - 1, :, at]
            if z < planes - 1:
                near = near + g_ref[z + 1, :, at]
            l_ref[z, :, at] = b_ref[z, :, at] - (centre * x - near)
            before, here = here, after


def edges(i_ref, yb_ref, ya_ref, xh_ref, l_ref, gram_ref):
    planes, rows, width = l_ref.shape
    chunks = width // LANES
    row = lax.broadcasted_iota(jnp.int32, (rows, LANES), 0)
    low = lax.broadcasted_iota(jnp.int32, (rows, LANES), 1) < LANES // 2
    gram = jnp.zeros((LANES, LANES), jnp.float32)
    for z in range(planes):
        tiles = []
        for t in range(chunks):
            at = pl.ds(t * LANES, LANES)
            add = jnp.where(row == 0, yb_ref[z, :, at], 0.0)
            add = jnp.where(row == rows - 1, ya_ref[z, :, at], add)
            value = i_ref[z, :, at] + add
            if t == 0:
                value = value + jnp.where(low, xh_ref[z], 0.0)
            if t == chunks - 1:
                value = value + jnp.where(low, 0.0, xh_ref[z])
            l_ref[z, :, at] = value
            tiles.append(value)
        if 0 < z < planes - 1:
            gram = gram + split_gram(tiles)
    gram_ref[...] = gram


def outer(which, l_ref, h_ref, g_ref, r_ref, o_ref):
    z = outer_planes(l_ref.shape[0])[which]
    tiles = []
    for t in range(l_ref.shape[2] // LANES):
        at = pl.ds(t * LANES, LANES)
        value = l_ref[z, :, at] + h_ref[0, :, at]
        r_ref[0, :, at] = value
        tiles.append(value)
    gram = g_ref[...] + split_gram(tiles)
    o_ref[...] = pack_gram(gram) if which else gram


def final(cells, p_ref, l_ref, first_ref, second_ref, n_ref, m_ref, buf, gram, sem):
    planes, rows, width = l_ref.shape
    half, quarter = LANES // 2, LANES // 4
    mean = p_ref[...] / jnp.float32(cells)
    row = lax.broadcasted_iota(jnp.int32, (quarter, LANES), 0)
    lane = lax.broadcasted_iota(jnp.int32, (quarter, LANES), 1)
    own = (lane == row) | (lane == row + half + quarter)
    diagonal = jnp.sum(jnp.where(own, mean, 0.0), axis=0, keepdims=True)
    diagonal = diagonal + half_roll(diagonal)
    scale = jnp.broadcast_to(lax.rsqrt(diagonal + 1e-06), (rows, LANES))
    first, second = outer_planes(planes)
    sources = [(z, l_ref.at[z]) for z in range(1, planes - 1)]
    sources += [(first, first_ref.at[0]), (second, second_ref.at[0])]
    copies = []
    for k, (z, source) in enumerate(sources):
        for t in range(width // LANES):
            at = pl.ds(t * LANES, LANES)
            buf[k, :, at] = source[:, at] * scale
        copies.append(pltpu.make_async_copy(buf.at[k], n_ref.at[z], sem.at[k]))
        copies[-1].start()
    square = jnp.concatenate([mean[:, :half], half_roll(mean)[:, :half]], axis=0)
    gram[...] = 0.5 * (square + square.T)
    copies.append(pltpu.make_async_copy(gram, m_ref, sem.at[planes]))
    copies[-1].start()
    for copy in copies:
        copy.wait()


def call(body, outs, cost, limit=16 << 20, **kwargs):
    return pl.pallas_call(
        body,
        out_shape=outs,
        cost_estimate=pl.CostEstimate(flops=cost, bytes_accessed=1 << 20, transcendentals=0),
        compiler_params=pltpu.CompilerParams(vmem_limit_bytes=limit),
        **kwargs,
    )


def z_exchange(array, turn):
    peers = lax.axis_size("gz")
    moves = [(z, (z + (1 if (z + turn) % 2 == 0 else -1)) % peers) for z in range(peers)]
    return lax.ppermute(array, "gz", moves)


def local(rhs, guess, shifts):
    z_cells, y_cells, lane_count = guess.shape
    columns = shifts.shape[0]
    x_cells = lane_count // columns
    f32 = jnp.float32
    whole = jax.ShapeDtypeStruct(guess.shape, f32)
    face = jax.ShapeDtypeStruct((1, y_cells, lane_count), f32)
    square = jax.ShapeDtypeStruct((LANES, LANES), f32)
    packed = jax.ShapeDtypeStruct((columns // 2, LANES), f32)
    in_vmem = pltpu.VMEM((1, y_cells, lane_count), f32)
    first, second = call(
        z_faces,
        (in_vmem, in_vmem),
        1 << 20,
        limit=60 << 20,
        in_specs=[HBM],
        out_specs=[VMEM] * 2,
        scratch_shapes=[pltpu.SemaphoreType.DMA((2,)), pltpu.SMEM((1,), jnp.int32)],
    )(guess)
    first = z_exchange(first, 0)
    second = z_exchange(second, 1)
    in_vmem = pltpu.VMEM(guess.shape, f32)
    guess, rhs = call(
        load,
        (in_vmem, in_vmem),
        1 << 20,
        limit=60 << 20,
        in_specs=[HBM] * 2,
        out_specs=[VMEM] * 2,
        scratch_shapes=[pltpu.SemaphoreType.DMA((2,))],
    )(guess, rhs)
    last, initial = faces(guess, 1, 1)
    y_before = ring(last, "gy", 1)
    y_after = ring(initial, "gy", -1)
    last, initial = faces(guess, 2, columns)
    if lax.axis_size("gx") == 2:
        x_halos = ring(jnp.concatenate([last, initial], axis=2), "gx", 1)
    else:
        x_halos = jnp.concatenate(
            [ring(last, "gx", 1), ring(initial, "gx", -1)], axis=2
        )
    centre = jnp.tile(6.0 + shifts, LANES // columns)[None]
    left = call(inside, whole, 1 << 24, in_specs=[VMEM] * 3, out_specs=VMEM)(guess, rhs, centre)
    left, gram = call(
        edges,
        (whole, square),
        1 << 24,
        in_specs=[VMEM] * 4,
        out_specs=[VMEM] * 2,
        input_output_aliases={0: 0},
    )(left, y_before, y_after, x_halos)
    first, gram = call(
        functools.partial(outer, 0),
        (face, square),
        1 << 22,
        in_specs=[VMEM] * 3,
        out_specs=[VMEM] * 2,
    )(left, first, gram)
    second, total = call(
        functools.partial(outer, 1),
        (face, packed),
        1 << 22,
        in_specs=[VMEM] * 3,
        out_specs=[VMEM] * 2,
    )(left, second, gram)
    total = sum_over_all(total)
    total_cells = z_cells * y_cells * x_cells * lax.axis_size(AXES)
    return call(
        functools.partial(final, total_cells),
        (whole, jax.ShapeDtypeStruct((columns, columns), f32)),
        1 << 22,
        in_specs=[VMEM] * 4,
        out_specs=[HBM] * 2,
        scratch_shapes=[
            pltpu.VMEM(guess.shape, f32),
            pltpu.VMEM((columns, columns), f32),
            pltpu.SemaphoreType.DMA((z_cells + 1,)),
        ],
    )(total, left, first, second)


def solution(mesh):
    placed = (P("gz", "gy", "gx"), P("gz", "gy", "gx"), P())
    return jax.shard_map(
        local, mesh=mesh, in_specs=placed, out_specs=(P("gz", "gy", "gx"), P()), check_vma=False
    )
```
